512 devices in a mesh: ex: 32 (over x, z), feat: 16 (over y, core).
Axes of the slice: x: 4, y: 8, z: 8, core: 2. Of those that a mesh axis runs over, the one named last changes fastest.
Arguments:
- pooled: bfloat16 [65536, 8192], P('ex', 'feat'), may hold values from -6 to 6
- labels: int32 [65536], P('ex'), may hold values from 0 to 1
- sign_bits: int32 [65536], P('ex'), may hold values from 0 to 1
- margins_old: float32 [65536], P('ex'), may hold values from -8 to 8
- direction: float32 [8192], P(('feat', 'ex')), may hold values from -0.0625 to 0.0625
- sample_rows: int32 [1024], replicated, may hold values from 0 to 65535
Outputs:
- margins: float32 [65536], P('ex')
- gradient: float32 [8192], P(('feat', 'ex'))
- sketch: float32 [1024, 8192], P('ex', 'feat')
The draws below stay inside these ranges and needn't reach their ends.
Inputs may be any that keep to these rules, and one draw needn't show every extreme that they name: `sample_rows`: indices are drawn independently, repeats possible.
All inputs are finite; a program needn't handle non-finite values.
Results may differ from the reference program's by a relative error of at most 0.0033.
Values may be sent and summed in bfloat16 or wider, within the bound.
A program may use at most 64 MiB of HBM per device.

```python
import math
import jax
import jax.numpy as jnp
from jax import lax

F = 8192
M = 1024
N = 65536


def plant(values, stream_key, smallest, top_value):
    shape = values.shape
    index_at = [jax.random.randint(jax.random.fold_in(stream_key, axis), (), 0, shape[axis]) for axis in range(len(shape))]
    values = values.at[tuple(index_at)].set(smallest)
    longest = shape.index(max(shape))
    index_at[longest] = (index_at[longest] + 1) % shape[longest]
    return values.at[tuple(index_at)].set(top_value)


def strengthened(values, key, source, target, parts, factor):
    owner, partner = [(jnp.arange(values.shape[dim]) // (values.shape[dim] // parts)).reshape([-1 if axis == dim else 1 for axis in range(values.ndim)]) for dim in (source, target)]
    chosen = jax.random.permutation(key, parts)[partner]
    strong = (owner == chosen) | (owner == (partner + parts // 2) % parts)
    return jnp.where(strong, factor * values, values)


def level_of(own_key, extent, shards, smallest, high):
    def one(axis_at, parts):
        draws = jax.random.uniform(jax.random.fold_in(jax.random.fold_in(own_key, 6), axis_at), (parts,), jnp.float32, smallest / len(shards), high / len(shards))
        return jnp.repeat(jnp.exp(draws), extent[axis_at] // parts).reshape((-1,) + (1,) * (len(extent) - axis_at - 1))

    gain = one(*shards[0])
    for cut in shards[1:]:
        gain = gain * one(*cut)
    return gain


def gaussian(key, extent, spread, most, shards=(), kind=jnp.bfloat16):
    drawn = spread * jax.random.normal(key, extent, jnp.float32)
    if shards:
        drawn = drawn * level_of(key, extent, shards, -0.22, 0.18)
    return jnp.clip(drawn, -most, most).astype(kind)


def gaussian_with(key, dims, width, reach, pieces, heavy, held_as=jnp.bfloat16):
    result = width * jax.random.normal(key, dims, jnp.float32)
    if pieces:
        result = result * level_of(key, dims, pieces, -0.22, 0.18)
    return jnp.clip(strengthened(result, jax.random.fold_in(key, 3), *heavy), -reach, reach).astype(held_as)


def setup_inputs(seed: int = 0) -> dict:
    arg_keys = jax.random.split(jax.random.key(seed), 7)
    return {
        "pooled": gaussian_with(arg_keys[0], (N, F), 1.0, 6.0, ((0, 32), (1, 16)), (0, 1, 32, 2.75)),
        "labels": plant(jax.random.randint(arg_keys[1], (N,), 0, 2), jax.random.fold_in(arg_keys[1], 1), 0, 1).astype(jnp.int32),
        "sign_bits": plant(jax.random.randint(arg_keys[2], (N,), 0, 2), jax.random.fold_in(arg_keys[2], 1), 0, 1).astype(jnp.int32),
        "margins_old": gaussian(arg_keys[3], (N,), 2.0, 8.0, ((0, 32),), jnp.float32),
        "direction": gaussian(arg_keys[4], (F,), F ** -0.5, 0.0625, ((0, 512),), jnp.float32),
        "sample_rows": plant(jax.random.randint(arg_keys[5], (M,), 0, N), jax.random.fold_in(arg_keys[5], 1), 0, N - 1).astype(jnp.int32),
    }


col_block = 512

def walsh_rows(column_part):
    row_total = column_part.shape[0]
    half_span = 1
    while half_span < row_total:
        shaped = column_part.reshape(row_total // (2 * half_span), 2, half_span, column_part.shape[1])
        upper_half = shaped[:, 0]
        lower_half = shaped[:, 1]
        column_part = jnp.stack([upper_half + lower_half, upper_half - lower_half], axis=1).reshape(row_total, column_part.shape[1])
        half_span = half_span * 2
    return column_part

def reference(pooled, labels, sign_bits, margins_old, direction, sample_rows):
    step_dir = direction.astype(jnp.bfloat16)
    margins = margins_old + jnp.dot(pooled, step_dir, preferred_element_type=jnp.float32)
    residual = jax.nn.sigmoid(margins) - labels.astype(jnp.float32)
    weight = jnp.sqrt(jax.nn.sigmoid(margins) * jax.nn.sigmoid(-margins))
    gradient = jnp.dot(residual.astype(jnp.bfloat16), pooled, preferred_element_type=jnp.float32) / math.sqrt(N)
    scale_rows = (2 * sign_bits - 1).astype(jnp.float32) * weight
    weighted = (pooled * scale_rows[:, None]).astype(jnp.bfloat16)
    stacked = weighted.reshape(N, F // col_block, col_block).transpose(1, 0, 2)

    def one_block(column_part):
        return walsh_rows(column_part.astype(jnp.float32))[sample_rows]
    picked = lax.map(one_block, stacked)
    sketch = picked.transpose(1, 0, 2).reshape(M, F) / math.sqrt(M)
    return (margins, gradient, sketch)
```

```python
import jax
import jax.numpy as jnp
from jax import lax
from jax.experimental import pallas as pl
from jax.experimental.pallas import tpu as pltpu
from jax.sharding import PartitionSpec as P

NX, NZ, NF = 4, 8, 16
ROWS, COLS, SAMPLES, LANES = 2048, 512, 1024, 128
HALF = COLS // 2
BLOCKS = ROWS // LANES
OWNED = SAMPLES // (NX * NZ)
OFFSETS = (4, 3, 5, 2, 6, 1, 7, 0)
F32, BF16 = jnp.float32, jnp.bfloat16
MESH = pl.DeviceIdType.MESH


def parity_sign(ids, mask):
    return 1 - 2 * jnp.bitwise_and(lax.population_count(jnp.bitwise_and(ids, mask)), 1)


def kernel(
    pooled_hbm, labels_hbm, bits_hbm, old_hbm, dir_hbm, rows_hbm,
    margins_out, grad_out, sketch_out,
    pooled, labels, bits, old, own_dir, rows,
    ids, table, weighted, zdir, xdir, terms,
    xgrad_send, xgrad, zgrad_send, zgrad,
    keep_a, keep_b, send_a, send_b, got_a, got_b,
    second_a, second_b, last_a, last_b, zsend, zgot,
    in_sem, zdir_sem, xdir_sem, terms_sem, xgrad_sem, zgrad_sem,
    first_sem, second_sem, zsketch_sem,
):
    ex = lax.axis_index("ex")
    feat = lax.axis_index("feat")
    x, z = ex // NZ, ex % NZ
    flip = x + 1 - 2 * (x % 2)
    back = NX - 1 - x
    across = (x + 2) % NX
    groups = (x, flip, back, across)

    def at_x(other):
        return {"ex": other * NZ + z}

    def at_z(step):
        return {"ex": x * NZ + (z + step) % NZ}

    def at_feat(step):
        return {"feat": (feat + step) % NF}

    loads = [
        pltpu.make_async_copy(src, dst, in_sem.at[i])
        for i, (src, dst) in enumerate(
            ((dir_hbm, own_dir), (rows_hbm, rows), (pooled_hbm, pooled), (old_hbm, old), (labels_hbm, labels), (bits_hbm, bits))
        )
    ]
    for load in loads:
        load.start()

    barrier = pltpu.get_barrier_semaphore()
    for step in range(1, NX):
        pl.semaphore_signal(barrier, inc=1, device_id=at_x((x + step) % NX), device_id_type=MESH)
    for step in range(1, NZ):
        pl.semaphore_signal(barrier, inc=1, device_id=at_z(step), device_id_type=MESH)
    for step in range(1, NF):
        pl.semaphore_signal(barrier, inc=1, device_id=at_feat(step), device_id_type=MESH)

    def remote(src, dst, sems, slot, device):
        return pltpu.make_async_remote_copy(
            src_ref=src, dst_ref=dst, send_sem=sems.at[0, slot], recv_sem=sems.at[1, slot], device_id=device, device_id_type=MESH
        )

    loads[0].wait()
    lane_row = lax.broadcasted_iota(jnp.int32, (1, LANES), 1)
    spread = jnp.concatenate([own_dir[...]] * NZ, axis=1)
    zdir[0] = jnp.where(lane_row // 16 == z, spread, 0.0)

    loads[1].wait()
    turned = jnp.transpose(rows[...])
    for t in range(SAMPLES // LANES):
        ids[t * LANES : (t + 1) * LANES, :] = jnp.broadcast_to(turned[:, t : t + 1], (LANES, LANES))

    def table_block(index):
        part, step = index // NZ, index % NZ
        offset = jnp.where(step % 2 == 0, NZ // 2 + step // 2, NZ // 2 - (step + 1) // 2)
        owner = jnp.where(part == 0, x, jnp.where(part == 1, flip, jnp.where(part == 2, back, across)))
        start = pl.multiple_of(owner * (NZ * OWNED) + (z + offset) % NZ * OWNED, OWNED)
        there = pl.multiple_of(step * (NX * OWNED) + part * OWNED, OWNED)
        wanted = ids[pl.ds(start, OWNED), :]
        lanes = lax.broadcasted_iota(jnp.int32, (OWNED, LANES), 1)
        signs = [None] * BLOCKS
        signs[0] = parity_sign(wanted, ex * ROWS + lanes).astype(F32).astype(BF16)
        for bit in range(4):
            this = (1 - 2 * jnp.bitwise_and(jnp.right_shift(wanted, 7 + bit), 1)).astype(F32).astype(BF16)
            for low in range(1 << bit):
                signs[low + (1 << bit)] = signs[low] * this
        for block in range(BLOCKS):
            table[pl.ds(there, OWNED), block * LANES : (block + 1) * LANES] = signs[block]

    pl.loop(0, 8)(table_block)
    pl.semaphore_wait(barrier, NX + NZ + NF - 3)

    zdir_copies = [remote(zdir.at[0], zdir.at[step], zdir_sem, step, at_z(step)) for step in range(1, NZ)]
    for copy in zdir_copies:
        copy.start()
    pl.loop(8, 24)(table_block)
    for copy in zdir_copies:
        copy.wait_recv()
    row = zdir[0]
    for step in range(1, NZ):
        row = row + zdir[step]
    xdir[x] = row
    xdir_copies = [remote(xdir.at[x], xdir.at[x], xdir_sem, step, at_x((x + step) % NX)) for step in range(1, NX)]
    for copy in xdir_copies:
        copy.start()
    pl.loop(24, 32)(table_block)
    loads[2].wait()
    for copy in xdir_copies:
        copy.wait_recv()

    step_dir = jnp.concatenate([xdir[i] for i in range(NX)], axis=1).astype(BF16)
    step_dir = jnp.broadcast_to(step_dir, (BLOCKS, COLS))
    block_row = lax.broadcasted_iota(jnp.int32, (BLOCKS, LANES), 0)
    partial = jnp.zeros((BLOCKS, LANES), F32)
    for block in range(BLOCKS):
        here = lax.dot_general(
            step_dir,
            pooled[block * LANES : (block + 1) * LANES, :],
            (((1,), (1,)), ((), ())),
            preferred_element_type=F32,
        )
        partial = jnp.where(block_row == block, here, partial)
    terms[feat] = partial.astype(BF16)
    terms_copies = [remote(terms.at[feat], terms.at[feat], terms_sem, step, at_feat(step)) for step in range(1, NF)]
    for copy in terms_copies:
        copy.start()
    for load in loads[3:]:
        load.wait()
    for copy in terms_copies:
        copy.wait_recv()
    total = terms[0].astype(F32)
    for i in range(1, NF):
        total = total + terms[i].astype(F32)
    margins = old[...] + total
    margins_out[...] = margins
    decay = jnp.exp(-jnp.abs(margins))
    likely = 1.0 / (1.0 + decay)
    rare = decay * likely
    weight = jnp.sqrt(likely * rare)
    residual = jnp.where(margins >= 0, likely, rare) - labels[...].astype(F32)
    scale = (2 * bits[...] - 1).astype(F32) * weight
    columns = jnp.transpose(scale)
    for block in range(BLOCKS):
        at = slice(block * LANES, (block + 1) * LANES)
        weighted[at, :] = (pooled[at, :].astype(F32) * columns[:, block : block + 1]).astype(BF16)

    def compute(pair):
        at = slice(pair * 2 * NX * OWNED, (pair + 1) * 2 * NX * OWNED)
        left = jnp.dot(table[at, :], weighted[:, :HALF], preferred_element_type=F32)
        right = jnp.dot(table[at, :], weighted[:, HALF:], preferred_element_type=F32)
        for k in range(2):
            c = 2 * pair + k
            g = [slice((k * NX + i) * OWNED, (k * NX + i + 1) * OWNED) for i in range(NX)]
            keep_a[c, :OWNED, :] = left[g[0]]
            keep_a[c, OWNED:, :] = left[g[2]]
            send_a[c, :OWNED, :] = left[g[1]].astype(BF16)
            send_a[c, OWNED:, :] = left[g[3]].astype(BF16)
            keep_b[c] = right[g[0].start : g[1].stop]
            send_b[c] = right[g[2].start : g[3].stop].astype(BF16)

    pending = []

    def launch(*copies):
        for copy in copies:
            copy.start()
            pending.append(copy)
        return copies

    def first(c):
        return launch(
            remote(send_a.at[c], got_a.at[c], first_sem, 2 * c, at_x(flip)),
            remote(send_b.at[c], got_b.at[c], first_sem, 2 * c + 1, at_x(back)),
        )

    def second(c, copies):
        for copy in copies:
            copy.wait_recv()
        second_a[c] = (keep_a[c, OWNED:, :] + got_a[c, OWNED:, :].astype(F32)).astype(BF16)
        second_b[c] = (keep_b[c, OWNED:, :] + got_b[c, OWNED:, :].astype(F32)).astype(BF16)
        return launch(
            remote(second_a.at[c], last_a.at[c], second_sem, 2 * c, at_x(back)),
            remote(second_b.at[c], last_b.at[c], second_sem, 2 * c + 1, at_x(flip)),
        )

    def third(c, copies):
        for copy in copies:
            copy.wait_recv()
        sum_a = keep_a[c, :OWNED, :] + got_a[c, :OWNED, :].astype(F32) + last_a[c].astype(F32)
        sum_b = keep_b[c, :OWNED, :] + got_b[c, :OWNED, :].astype(F32) + last_b[c].astype(F32)
        if OFFSETS[c] == 0:
            return sum_a, sum_b
        zsend[c, :, :HALF] = sum_a.astype(BF16)
        zsend[c, :, HALF:] = sum_b.astype(BF16)
        return launch(remote(zsend.at[c], zgot.at[c], zsketch_sem, c, at_z(OFFSETS[c])))

    ones, twos, threes = {}, {}, {}
    compute(0)
    ones[0], ones[1] = first(0), first(1)
    compute(1)
    ones[2], ones[3] = first(2), first(3)

    flat = jnp.concatenate([residual[i : i + 1, :] for i in range(BLOCKS)], axis=1).astype(BF16)
    grad = jnp.dot(jnp.broadcast_to(flat, (8, ROWS)), pooled[...], preferred_element_type=F32)[0:1, :]
    for i in range(NX):
        xgrad_send[i] = grad[:, i * LANES : (i + 1) * LANES]
    xgrad_copies = launch(*(
        remote(xgrad_send.at[(x + step) % NX], xgrad.at[step], xgrad_sem, step, at_x((x + step) % NX)) for step in range(1, NX)
    ))

    compute(2)
    compute(3)
    for c in range(NZ):
        twos[c] = second(c, ones[c])
        if c + 4 < NZ:
            ones[c + 4] = first(c + 4)
        if c == 1:
            for copy in xgrad_copies:
                copy.wait_recv()
            part = xgrad_send[x]
            for step in range(1, NX):
                part = part + xgrad[step]
            zgrad_send[...] = part
            zgrad_copies = launch(*(remote(zgrad_send, zgrad.at[step], zgrad_sem, step, at_z(step)) for step in range(1, NZ)))
        if c >= 2:
            threes[c - 2] = third(c - 2, twos[c - 2])
    threes[NZ - 2] = third(NZ - 2, twos[NZ - 2])

    for copy in zgrad_copies:
        copy.wait_recv()
    part = zgrad_send[...]
    for step in range(1, NZ):
        part = part + zgrad[step]
    grad_out[...] = pltpu.roll(part, (NZ - z) * 16 % LANES, 1) * (1.0 / 256.0)

    sum_a, sum_b = third(NZ - 1, twos[NZ - 1])
    for c in range(NZ - 1):
        threes[c][0].wait_recv()
        sum_a = sum_a + zgot[c, :, :HALF].astype(F32)
        sum_b = sum_b + zgot[c, :, HALF:].astype(F32)
    sketch_out[:, :HALF] = sum_a * (1.0 / 32.0)
    sketch_out[:, HALF:] = sum_b * (1.0 / 32.0)

    for copy in (*zdir_copies, *xdir_copies, *terms_copies, *pending):
        copy.wait_send()


def on_device(pooled, labels, sign_bits, margins_old, direction, sample_rows):
    dma = pltpu.SemaphoreType.DMA
    vmem = pltpu.VMEM
    margins, grad, sketch = pl.pallas_call(
        kernel,
        out_shape=(
            jax.ShapeDtypeStruct((BLOCKS, LANES), F32),
            jax.ShapeDtypeStruct((1, LANES), F32),
            jax.ShapeDtypeStruct((OWNED, COLS), F32),
        ),
        in_specs=[pl.BlockSpec(memory_space=pl.ANY)] * 6,
        out_specs=[pl.BlockSpec(memory_space=vmem)] * 3,
        scratch_shapes=[
            vmem((ROWS, COLS), BF16),
            vmem((BLOCKS, LANES), jnp.int32),
            vmem((BLOCKS, LANES), jnp.int32),
            vmem((BLOCKS, LANES), F32),
            vmem((1, 16), F32),
            vmem((SAMPLES // LANES, LANES), jnp.int32),
            vmem((SAMPLES, LANES), jnp.int32),
            vmem((SAMPLES, ROWS), BF16),
            vmem((ROWS, COLS), BF16),
            vmem((NZ, 1, LANES), F32),
            vmem((NX, 1, LANES), F32),
            vmem((NF, BLOCKS, LANES), BF16),
            vmem((NX, 1, LANES), F32),
            vmem((NX, 1, LANES), F32),
            vmem((1, LANES), F32),
            vmem((NZ, 1, LANES), F32),
            vmem((NZ, 2 * OWNED, HALF), F32),
            vmem((NZ, 2 * OWNED, HALF), F32),
            vmem((NZ, 2 * OWNED, HALF), BF16),
            vmem((NZ, 2 * OWNED, HALF), BF16),
            vmem((NZ, 2 * OWNED, HALF), BF16),
            vmem((NZ, 2 * OWNED, HALF), BF16),
            vmem((NZ, OWNED, HALF), BF16),
            vmem((NZ, OWNED, HALF), BF16),
            vmem((NZ, OWNED, HALF), BF16),
            vmem((NZ, OWNED, HALF), BF16),
            vmem((NZ, OWNED, COLS), BF16),
            vmem((NZ, OWNED, COLS), BF16),
            dma((6,)),
            dma((2, NZ)),
            dma((2, NX)),
            dma((2, NF)),
            dma((2, NX)),
            dma((2, NZ)),
            dma((2, 2 * NZ)),
            dma((2, 2 * NZ)),
            dma((2, NZ)),
        ],
        compiler_params=pltpu.CompilerParams(collective_id=0, has_side_effects=True),
        name="newton_sketch",
    )(
        pooled,
        labels.reshape(BLOCKS, LANES),
        sign_bits.reshape(BLOCKS, LANES),
        margins_old.reshape(BLOCKS, LANES),
        direction.reshape(1, 16),
        sample_rows.reshape(SAMPLES // LANES, LANES),
    )
    return margins.reshape(ROWS), grad[0, :16], sketch


def solution(mesh):
    return jax.shard_map(
        on_device,
        mesh=mesh,
        in_specs=(P("ex", "feat"), P("ex"), P("ex"), P("ex"), P(("feat", "ex")), P()),
        out_specs=(P("ex"), P(("feat", "ex")), P("ex", "feat")),
        check_vma=False,
    )
```

```python
import jax
import jax.numpy as jnp
from jax import lax
from jax.experimental import pallas as pl
from jax.experimental.pallas import tpu as pltpu
from jax.sharding import PartitionSpec as P

NX, NZ, NF = 4, 8, 16
ROWS, COLS, SAMPLES, LANES = 2048, 512, 1024, 128
HALF = COLS // 2
BLOCKS = ROWS // LANES
OWNED = SAMPLES // (NX * NZ)
QUARTER = LANES
F32, BF16 = jnp.float32, jnp.bfloat16
MESH = pl.DeviceIdType.MESH


def parity_sign(ids, mask):
    return 1 - 2 * jnp.bitwise_and(lax.population_count(jnp.bitwise_and(ids, mask)), 1)


FAR_FIRST = (4, 3, 5, 2, 6, 1, 7)


def kernel(
    pooled_hbm, labels_hbm, bits_hbm, old_hbm, dir_hbm, rows_hbm,
    margins_out, grad_out, sketch_out,
    pooled, labels, bits, old, own_dir, rows,
    ids, table, weighted, zdir, xdir, terms,
    xgrad_send, xgrad, zgrad_send, zgrad,
    keep_a, keep_b, keep_c, keep_d, pair_send, pair_got,
    first_send, first_got, second_send, second_got, wide_send, wide_got, slim_send, slim_got,
    in_sem, zdir_sem, xdir_sem, terms_sem, xgrad_sem, zgrad_sem,
    pair_sem, first_sem, second_sem, wide_sem, slim_sem,
):
    ex = lax.axis_index("ex")
    feat = lax.axis_index("feat")
    x, z = ex // NZ, ex % NZ
    flip = x + 1 - 2 * (x % 2)
    back = NX - 1 - x
    across = (x + 2) % NX
    away = 2 * (z % 2) - 1

    def at_x(other):
        return {"ex": other * NZ + z}

    def at_z(step):
        return {"ex": x * NZ + (z + step + 2 * NZ) % NZ}

    def at_feat(step, other):
        return {"feat": (feat // 2 + step) % NZ * 2 + (feat % 2 + other) % 2}

    near = [(step, other) for step in FAR_FIRST for other in range(2)] + [(0, 1)]
    loads = [
        pltpu.make_async_copy(src, dst, in_sem.at[i])
        for i, (src, dst) in enumerate(
            ((dir_hbm, own_dir), (rows_hbm, rows), (pooled_hbm, pooled), (old_hbm, old), (labels_hbm, labels), (bits_hbm, bits))
        )
    ]
    loads[0].start()
    barrier = pltpu.get_barrier_semaphore()
    for step in FAR_FIRST:
        pl.semaphore_signal(barrier, inc=1, device_id=at_z(step), device_id_type=MESH)
    for step in (2, 1, 3):
        pl.semaphore_signal(barrier, inc=1, device_id=at_x((x + step) % NX), device_id_type=MESH)
    for step, other in near:
        pl.semaphore_signal(barrier, inc=1, device_id=at_feat(step, other), device_id_type=MESH)
    for load in loads[1:]:
        load.start()

    def send(src, dst, sems, device, group=0):
        pltpu.make_async_remote_copy(
            src_ref=src, dst_ref=dst, send_sem=sems.at[0], recv_sem=sems.at[1 + group], device_id=device, device_id_type=MESH
        ).start()

    def landed(ref, sems, group=0):
        pltpu.make_async_copy(ref, ref, sems.at[1 + group]).wait()

    def left(ref, sems):
        pltpu.make_async_copy(ref, ref, sems.at[0]).wait()

    loads[0].wait()
    lane_row = lax.broadcasted_iota(jnp.int32, (1, LANES), 1)
    spread = jnp.concatenate([own_dir[...]] * NZ, axis=1)
    zdir[0] = jnp.where(lane_row // 16 == z, spread, 0.0)
    pl.semaphore_wait(barrier, NX + NZ + NF - 3)
    for step in FAR_FIRST:
        send(zdir.at[0], zdir.at[step], zdir_sem, at_z(step))
    loads[1].wait()
    turned = jnp.transpose(rows[...])
    for t in range(SAMPLES // LANES):
        ids[t * LANES : (t + 1) * LANES, :] = jnp.broadcast_to(turned[:, t : t + 1], (LANES, LANES))

    def table_block(index):
        part, step = index // NZ, index % NZ
        offset = away * jnp.where(step % 2 == 1, (NZ - 1 - step) // 2, -((NZ - step) // 2))
        owner = jnp.where(part == 0, x, jnp.where(part == 1, flip, jnp.where(part == 2, back, across)))
        start = pl.multiple_of(owner * (NZ * OWNED) + (z + offset + NZ) % NZ * OWNED, OWNED)
        there = pl.multiple_of(step * (NX * OWNED) + part * OWNED, OWNED)
        wanted = ids[pl.ds(start, OWNED), :]
        lanes = lax.broadcasted_iota(jnp.int32, (OWNED, LANES), 1)
        signs = [None] * BLOCKS
        signs[0] = parity_sign(wanted, ex * ROWS + lanes).astype(F32).astype(BF16)
        for bit in range(4):
            this = (1 - 2 * jnp.bitwise_and(jnp.right_shift(wanted, 7 + bit), 1)).astype(F32).astype(BF16)
            for low in range(1 << bit):
                signs[low + (1 << bit)] = signs[low] * this
        for block in range(BLOCKS):
            table[pl.ds(there, OWNED), block * LANES : (block + 1) * LANES] = signs[block]

    pl.loop(0, 20)(table_block)
    landed(zdir.at[1:], zdir_sem)
    row = zdir[0]
    for step in range(1, NZ):
        row = row + zdir[step]
    xdir[x] = row
    for step in (2, 1, 3):
        send(xdir.at[x], xdir.at[x], xdir_sem, at_x((x + step) % NX))
    pl.loop(20, 32)(table_block)
    loads[2].wait()
    landed(xdir.at[1:], xdir_sem)
    step_dir = jnp.concatenate([xdir[i] for i in range(NX)], axis=1).astype(BF16)
    step_dir = jnp.broadcast_to(step_dir, (BLOCKS, COLS))
    block_row = lax.broadcasted_iota(jnp.int32, (BLOCKS, LANES), 0)
    partial = jnp.zeros((BLOCKS, LANES), F32)
    for block in range(BLOCKS):
        here = lax.dot_general(
            step_dir,
            pooled[block * LANES : (block + 1) * LANES, :],
            (((1,), (1,)), ((), ())),
            preferred_element_type=F32,
        )
        partial = jnp.where(block_row == block, here, partial)
    terms[feat] = partial.astype(BF16)
    for step, other in near:
        send(terms.at[feat], terms.at[feat], terms_sem, at_feat(step, other))
    for load in loads[3:]:
        load.wait()
    landed(terms.at[1:], terms_sem)
    total = terms[0].astype(F32)
    for i in range(1, NF):
        total = total + terms[i].astype(F32)
    margins = old[...] + total
    margins_out[...] = margins
    decay = jnp.exp(-jnp.abs(margins))
    likely = 1.0 / (1.0 + decay)
    rare = decay * likely
    weight = jnp.sqrt(likely * rare)
    residual = jnp.where(margins >= 0, likely, rare) - labels[...].astype(F32)
    scale = (2 * bits[...] - 1).astype(F32) * weight
    columns = jnp.transpose(scale)
    for block in range(BLOCKS):
        at = slice(block * LANES, (block + 1) * LANES)
        weighted[at, :] = (pooled[at, :].astype(F32) * columns[:, block : block + 1]).astype(BF16)

    def launch_first(i):
        send(first_send.at[2 * i], first_got.at[2 * i], first_sem, at_x(flip), i)
        send(first_send.at[2 * i + 1], first_got.at[2 * i + 1], first_sem, at_x(back), i)

    def compute(pair):
        at = slice(pair * 2 * NX * OWNED, (pair + 1) * 2 * NX * OWNED)
        product = [
            jnp.dot(table[at, :], weighted[:, i * HALF : (i + 1) * HALF], preferred_element_type=F32) for i in range(2)
        ]
        sends = []
        for k in range(2):
            i = 2 * pair + k
            block = product[1][k * NX * OWNED : (k + 1) * NX * OWNED]
            for colour, keeps, keep, device in ((0, (1, 3, 5, 7), keep_c, at_z(-away)), (1, (2, 4, 6, 7), keep_d, at_z(away))):
                part = block[:, colour * QUARTER : (colour + 1) * QUARTER]
                if i in keeps:
                    keep[keeps.index(i)] = part
                else:
                    n = [j for j in range(NZ) if j not in keeps].index(i)
                    slot = 2 * n + colour
                    pair_send[slot] = part.astype(BF16)
                    sends.append((slot, n, device))
            block = product[0][k * NX * OWNED : (k + 1) * NX * OWNED]
            g = [slice(j * OWNED, (j + 1) * OWNED) for j in range(NX)]
            keep_a[i, :OWNED, :] = block[g[0], :QUARTER]
            keep_a[i, OWNED:, :] = block[g[2], :QUARTER]
            first_send[2 * i, :OWNED, :] = block[g[1], :QUARTER].astype(BF16)
            first_send[2 * i, OWNED:, :] = block[g[3], :QUARTER].astype(BF16)
            keep_b[i] = block[: 2 * OWNED, QUARTER:]
            first_send[2 * i + 1] = block[2 * OWNED :, QUARTER:].astype(BF16)
        for slot, n, device in sends:
            send(pair_send.at[slot], pair_got.at[slot], pair_sem, device, n)
        launch_first(2 * pair)
        launch_first(2 * pair + 1)

    def after_pair(n):
        landed(pair_got.at[2 * n : 2 * n + 2], pair_sem, n)
        i = NZ + n
        c, d = 2 * n, 2 * n + 1
        first_send[2 * i, :OWNED, :] = (keep_c[n, OWNED : 2 * OWNED, :] + pair_got[c, OWNED : 2 * OWNED, :].astype(F32)).astype(BF16)
        first_send[2 * i, OWNED:, :] = (keep_c[n, 3 * OWNED :, :] + pair_got[c, 3 * OWNED :, :].astype(F32)).astype(BF16)
        first_send[2 * i + 1] = (keep_d[n, 2 * OWNED :, :] + pair_got[d, 2 * OWNED :, :].astype(F32)).astype(BF16)
        launch_first(i)
        keep_a[i, :OWNED, :] = keep_c[n, :OWNED, :] + pair_got[c, :OWNED, :].astype(F32)
        keep_a[i, OWNED:, :] = keep_c[n, 2 * OWNED : 3 * OWNED, :] + pair_got[c, 2 * OWNED : 3 * OWNED, :].astype(F32)
        keep_b[i] = keep_d[n, : 2 * OWNED, :] + pair_got[d, : 2 * OWNED, :].astype(F32)

    def after_first(i):
        landed(first_got.at[2 * i : 2 * i + 2], first_sem, i)
        second_send[2 * i] = (keep_a[i, OWNED:, :] + first_got[2 * i, OWNED:, :].astype(F32)).astype(BF16)
        second_send[2 * i + 1] = (keep_b[i, OWNED:, :] + first_got[2 * i + 1, OWNED:, :].astype(F32)).astype(BF16)
        send(second_send.at[2 * i], second_got.at[2 * i], second_sem, at_x(back), i)
        send(second_send.at[2 * i + 1], second_got.at[2 * i + 1], second_sem, at_x(flip), i)

    def after_second(i):
        landed(second_got.at[2 * i : 2 * i + 2], second_sem, i)
        return (
            keep_a[i, :OWNED, :] + first_got[2 * i, :OWNED, :].astype(F32) + second_got[2 * i].astype(F32),
            keep_b[i, :OWNED, :] + first_got[2 * i + 1, :OWNED, :].astype(F32) + second_got[2 * i + 1].astype(F32),
        )

    def wide(i):
        sum_a, sum_b = after_second(i)
        wide_send[i, :, :QUARTER] = sum_a.astype(BF16)
        wide_send[i, :, QUARTER:] = sum_b.astype(BF16)
        offset = (NZ - 1 - i) // 2 if i % 2 else -((NZ - i) // 2)
        send(wide_send.at[i], wide_got.at[i], wide_sem, at_z(away * offset))

    def slim(n):
        sum_c, sum_d = after_second(NZ + n)
        slim_send[2 * n] = sum_c.astype(BF16)
        slim_send[2 * n + 1] = sum_d.astype(BF16)
        send(slim_send.at[2 * n], slim_got.at[2 * n], slim_sem, at_z(away * (NX - 1 - n)))
        send(slim_send.at[2 * n + 1], slim_got.at[2 * n + 1], slim_sem, at_z(-away * (NX - 1 - n)))

    compute(0)
    compute(1)
    compute(2)
    compute(3)
    flat = jnp.concatenate([residual[i : i + 1, :] for i in range(BLOCKS)], axis=1).astype(BF16)
    grad = jnp.dot(jnp.broadcast_to(flat, (8, ROWS)), pooled[...], preferred_element_type=F32)[0:1, :]
    for i in range(NX):
        xgrad_send[i] = grad[:, i * LANES : (i + 1) * LANES]
    for step in (2, 1, 3):
        send(xgrad_send.at[(x + step) % NX], xgrad.at[step], xgrad_sem, at_x((x + step) % NX))
    after_pair(0)
    after_first(0)
    after_first(1)
    after_pair(1)
    after_first(2)
    after_first(3)
    after_pair(2)
    after_first(4)
    after_first(5)
    after_pair(3)
    after_first(8)
    wide(0)
    after_first(6)
    after_first(7)
    wide(1)
    wide(2)
    after_first(9)
    wide(3)
    wide(4)
    landed(xgrad.at[1:], xgrad_sem)
    part = xgrad_send[x]
    for step in range(1, NX):
        part = part + xgrad[step]
    zgrad_send[...] = part
    for step in FAR_FIRST:
        send(zgrad_send, zgrad.at[step], zgrad_sem, at_z(step))
    after_first(10)
    slim(0)
    wide(5)
    wide(6)
    after_first(11)
    slim(1)
    slim(2)
    sum_a, sum_b = after_second(NZ - 1)
    sum_c, sum_d = after_second(NZ + NX - 1)
    landed(zgrad.at[1:], zgrad_sem)
    part = zgrad_send[...]
    for step in range(1, NZ):
        part = part + zgrad[step]
    grad_out[...] = pltpu.roll(part, (NZ - z) * 16 % LANES, 1)[:, :16] * (1.0 / 256.0)
    landed(wide_got, wide_sem)
    for i in range(NZ - 1):
        sum_a = sum_a + wide_got[i, :, :QUARTER].astype(F32)
        sum_b = sum_b + wide_got[i, :, QUARTER:].astype(F32)
    landed(slim_got, slim_sem)
    for n in range(NX - 1):
        sum_c = sum_c + slim_got[2 * n].astype(F32)
        sum_d = sum_d + slim_got[2 * n + 1].astype(F32)
    for i, part in enumerate((sum_a, sum_b, sum_c, sum_d)):
        sketch_out[:, i * QUARTER : (i + 1) * QUARTER] = part * (1.0 / 32.0)
    left(zdir.at[1:], zdir_sem)
    left(xdir.at[1:], xdir_sem)
    left(terms.at[1:], terms_sem)
    left(xgrad.at[1:], xgrad_sem)
    left(zgrad.at[1:], zgrad_sem)
    left(pair_send, pair_sem)
    left(first_send, first_sem)
    left(second_send, second_sem)
    left(wide_send, wide_sem)
    left(slim_send, slim_sem)


def put_out(margins, grad, sketch, margins_hbm, grad_hbm, sketch_hbm, sem):
    copies = [
        pltpu.make_async_copy(src, dst, sem.at[i])
        for i, (src, dst) in enumerate(((sketch, sketch_hbm), (margins, margins_hbm), (grad, grad_hbm)))
    ]
    for copy in copies:
        copy.start()
    for copy in copies:
        copy.wait()


def on_device(pooled, labels, sign_bits, margins_old, direction, sample_rows):
    dma = pltpu.SemaphoreType.DMA
    vmem = pltpu.VMEM
    margins, grad, sketch = pl.pallas_call(
        kernel,
        out_shape=(
            jax.ShapeDtypeStruct((BLOCKS, LANES), F32),
            jax.ShapeDtypeStruct((1, 16), F32),
            jax.ShapeDtypeStruct((OWNED, COLS), F32),
        ),
        in_specs=[pl.BlockSpec(memory_space=pl.ANY)] * 6,
        out_specs=[pl.BlockSpec(memory_space=vmem)] * 3,
        scratch_shapes=[
            vmem((ROWS, COLS), BF16),
            vmem((BLOCKS, LANES), jnp.int32),
            vmem((BLOCKS, LANES), jnp.int32),
            vmem((BLOCKS, LANES), F32),
            vmem((1, 16), F32),
            vmem((SAMPLES // LANES, LANES), jnp.int32),
            vmem((SAMPLES, LANES), jnp.int32),
            vmem((SAMPLES, ROWS), BF16),
            vmem((ROWS, COLS), BF16),
            vmem((NZ, 1, LANES), F32),
            vmem((NX, 1, LANES), F32),
            vmem((NF, BLOCKS, LANES), BF16),
            vmem((NX, 1, LANES), F32),
            vmem((NX, 1, LANES), F32),
            vmem((1, LANES), F32),
            vmem((NZ, 1, LANES), F32),
            vmem((NZ + NX, 2 * OWNED, QUARTER), F32),
            vmem((NZ + NX, 2 * OWNED, QUARTER), F32),
            vmem((NX, NX * OWNED, QUARTER), F32),
            vmem((NX, NX * OWNED, QUARTER), F32),
            vmem((2 * NX, NX * OWNED, QUARTER), BF16),
            vmem((2 * NX, NX * OWNED, QUARTER), BF16),
            vmem((2 * (NZ + NX), 2 * OWNED, QUARTER), BF16),
            vmem((2 * (NZ + NX), 2 * OWNED, QUARTER), BF16),
            vmem((2 * (NZ + NX), OWNED, QUARTER), BF16),
            vmem((2 * (NZ + NX), OWNED, QUARTER), BF16),
            vmem((NZ - 1, OWNED, 2 * QUARTER), BF16),
            vmem((NZ - 1, OWNED, 2 * QUARTER), BF16),
            vmem((2 * (NX - 1), OWNED, QUARTER), BF16),
            vmem((2 * (NX - 1), OWNED, QUARTER), BF16),
            dma((6,)),
            dma((2,)),
            dma((2,)),
            dma((2,)),
            dma((2,)),
            dma((2,)),
            dma((1 + NX,)),
            dma((1 + NZ + NX,)),
            dma((1 + NZ + NX,)),
            dma((2,)),
            dma((2,)),
        ],
        compiler_params=pltpu.CompilerParams(vmem_limit_bytes=40 << 20, collective_id=0, has_side_effects=True),
        name="newton_sketch",
    )(*(pltpu.with_memory_space_constraint(array, pltpu.HBM) for array in (
        pooled,
        labels.reshape(BLOCKS, LANES),
        sign_bits.reshape(BLOCKS, LANES),
        margins_old.reshape(BLOCKS, LANES),
        direction.reshape(1, 16),
        sample_rows.reshape(SAMPLES // LANES, LANES),
    )))
    margins, grad, sketch = pl.pallas_call(
        put_out,
        out_shape=(
            jax.ShapeDtypeStruct((BLOCKS, LANES), F32),
            jax.ShapeDtypeStruct((1, 16), F32),
            jax.ShapeDtypeStruct((OWNED, COLS), F32),
        ),
        in_specs=[pl.BlockSpec(memory_space=vmem)] * 3,
        out_specs=[pl.BlockSpec(memory_space=pl.ANY)] * 3,
        scratch_shapes=[dma((3,))],
        compiler_params=pltpu.CompilerParams(vmem_limit_bytes=1 << 20),
        name="put_out",
    )(margins, grad, sketch)
    return margins.reshape(ROWS), grad.reshape(16), sketch


def solution(mesh):
    return jax.shard_map(
        on_device,
        mesh=mesh,
        in_specs=(P("ex", "feat"), P("ex"), P("ex"), P("ex"), P(("feat", "ex")), P()),
        out_specs=(P("ex"), P(("feat", "ex")), P("ex", "feat")),
        check_vma=False,
    )
```

```python
import jax
import jax.numpy as jnp
from jax import lax
from jax.experimental import pallas as pl
from jax.experimental.pallas import tpu as pltpu
from jax.sharding import PartitionSpec as P

NX, NZ, NF = 4, 8, 16
ROWS, COLS, SAMPLES, LANES = 2048, 512, 1024, 128
HALF = COLS // 2
BLOCKS = ROWS // LANES
OWNED = SAMPLES // (NX * NZ)
QUARTER = LANES
F32, BF16 = jnp.float32, jnp.bfloat16
MESH = pl.DeviceIdType.MESH


def parity_sign(ids, mask):
    return 1 - 2 * jnp.bitwise_and(lax.population_count(jnp.bitwise_and(ids, mask)), 1)


FAR_FIRST = (4, 3, 5, 2, 6, 1, 7)
DIRECT = (0, 1, 2, 7)


def kernel(
    pooled_hbm, labels_hbm, bits_hbm, old_hbm, dir_hbm, rows_hbm,
    margins_out, grad_out, sketch_out,
    pooled, labels, bits, old, own_dir, rows,
    ids, table, weighted, zdir, xdir, terms,
    xgrad_send, xgrad, zgrad_send, zgrad,
    keep_a, keep_b, keep_c, keep_d, pair_send, pair_got,
    first_send, first_got, second_send, second_got, wide_send, wide_got, slim_send, slim_got,
    keep_w, direct_send, direct_got,
    in_sem, zdir_sem, xdir_sem, terms_sem, xgrad_sem, zgrad_sem,
    pair_sem, first_sem, second_sem, wide_sem, slim_sem, direct_sem,
):
    ex = lax.axis_index("ex")
    feat = lax.axis_index("feat")
    x, z = ex // NZ, ex % NZ
    flip = x + 1 - 2 * (x % 2)
    back = NX - 1 - x
    across = (x + 2) % NX
    away = 2 * (z % 2) - 1

    def at_x(other):
        return {"ex": other * NZ + z}

    def at_z(step):
        return {"ex": x * NZ + (z + step + 2 * NZ) % NZ}

    def at_feat(step, other):
        return {"feat": (feat // 2 + step) % NZ * 2 + (feat % 2 + other) % 2}

    near = [(step, other) for step in FAR_FIRST for other in range(2)] + [(0, 1)]
    loads = [
        pltpu.make_async_copy(src, dst, in_sem.at[i])
        for i, (src, dst) in enumerate(
            ((dir_hbm, own_dir), (rows_hbm, rows), (pooled_hbm, pooled), (old_hbm, old), (labels_hbm, labels), (bits_hbm, bits))
        )
    ]
    loads[0].start()
    barrier = pltpu.get_barrier_semaphore()
    for step in FAR_FIRST:
        pl.semaphore_signal(barrier, inc=1, device_id=at_z(step), device_id_type=MESH)
    for step in (2, 1, 3):
        pl.semaphore_signal(barrier, inc=1, device_id=at_x((x + step) % NX), device_id_type=MESH)
    for step, other in near:
        pl.semaphore_signal(barrier, inc=1, device_id=at_feat(step, other), device_id_type=MESH)
    for load in loads[1:]:
        load.start()

    def send(src, dst, sems, device, group=0):
        pltpu.make_async_remote_copy(
            src_ref=src, dst_ref=dst, send_sem=sems.at[0], recv_sem=sems.at[1 + group], device_id=device, device_id_type=MESH
        ).start()

    def landed(ref, sems, group=0):
        pltpu.make_async_copy(ref, ref, sems.at[1 + group]).wait()

    def left(ref, sems):
        pltpu.make_async_copy(ref, ref, sems.at[0]).wait()

    loads[0].wait()
    lane_row = lax.broadcasted_iota(jnp.int32, (1, LANES), 1)
    spread = jnp.concatenate([own_dir[...]] * NZ, axis=1)
    zdir[0] = jnp.where(lane_row // 16 == z, spread, 0.0)
    pl.semaphore_wait(barrier, NX + NZ + NF - 3)
    for step in FAR_FIRST:
        send(zdir.at[0], zdir.at[step], zdir_sem, at_z(step))
    loads[1].wait()
    turned = jnp.transpose(rows[...])
    for t in range(SAMPLES // LANES):
        ids[t * LANES : (t + 1) * LANES, :] = jnp.broadcast_to(turned[:, t : t + 1], (LANES, LANES))

    def table_block(index):
        part, step = index // NZ, index % NZ
        offset = away * jnp.where(step % 2 == 1, (NZ - 1 - step) // 2, -((NZ - step) // 2))
        owner = jnp.where(part == 0, x, jnp.where(part == 1, flip, jnp.where(part == 2, back, across)))
        start = pl.multiple_of(owner * (NZ * OWNED) + (z + offset + NZ) % NZ * OWNED, OWNED)
        there = pl.multiple_of(step * (NX * OWNED) + part * OWNED, OWNED)
        wanted = ids[pl.ds(start, OWNED), :]
        lanes = lax.broadcasted_iota(jnp.int32, (OWNED, LANES), 1)
        signs = [None] * BLOCKS
        signs[0] = parity_sign(wanted, ex * ROWS + lanes).astype(F32).astype(BF16)
        for bit in range(4):
            this = (1 - 2 * jnp.bitwise_and(jnp.right_shift(wanted, 7 + bit), 1)).astype(F32).astype(BF16)
            for low in range(1 << bit):
                signs[low + (1 << bit)] = signs[low] * this
        for block in range(BLOCKS):
            table[pl.ds(there, OWNED), block * LANES : (block + 1) * LANES] = signs[block]

    pl.loop(0, 20)(table_block)
    landed(zdir.at[1:], zdir_sem)
    row = zdir[0]
    for step in range(1, NZ):
        row = row + zdir[step]
    xdir[x] = row
    for step in (2, 1, 3):
        send(xdir.at[x], xdir.at[x], xdir_sem, at_x((x + step) % NX), step - 1)

    block_row = lax.broadcasted_iota(jnp.int32, (BLOCKS, LANES), 0)

    def product_of(other):
        part = jnp.broadcast_to(xdir[other], (BLOCKS, LANES)).astype(BF16)
        features = pl.ds(pl.multiple_of(other * LANES, LANES), LANES)
        result = jnp.zeros((BLOCKS, LANES), F32)
        for pair in range(BLOCKS // 2):
            here = lax.dot_general(
                part,
                pooled[pair * 2 * LANES : (pair + 1) * 2 * LANES, features],
                (((1,), (1,)), ((), ())),
                preferred_element_type=F32,
            )
            result = jnp.where(block_row == 2 * pair, here[:, :LANES], result)
            result = jnp.where(block_row == 2 * pair + 1, here[:, LANES:], result)
        return result

    pl.loop(20, 32)(table_block)
    loads[2].wait()
    partial = product_of(x)
    landed(xdir.at[0], xdir_sem, 0)
    partial = partial + product_of((x + NX - 1) % NX)
    landed(xdir.at[0], xdir_sem, 2)
    partial = partial + product_of((x + NX - 3) % NX)
    landed(xdir.at[0], xdir_sem, 1)
    partial = partial + product_of((x + NX - 2) % NX)
    terms[feat] = partial.astype(BF16)
    for step, other in near:
        send(terms.at[feat], terms.at[feat], terms_sem, at_feat(step, other))
    for load in loads[3:]:
        load.wait()
    landed(terms.at[1:], terms_sem)
    total = terms[0].astype(F32)
    for i in range(1, NF):
        total = total + terms[i].astype(F32)
    margins = old[...] + total
    margins_out[...] = margins
    decay = jnp.exp(-jnp.abs(margins))
    likely = 1.0 / (1.0 + decay)
    rare = decay * likely
    weight = jnp.sqrt(likely * rare)
    residual = jnp.where(margins >= 0, likely, rare) - labels[...].astype(F32)
    scale = (2 * bits[...] - 1).astype(F32) * weight
    columns = jnp.transpose(scale)
    for block in range(BLOCKS):
        at = slice(block * LANES, (block + 1) * LANES)
        weighted[at, :] = (pooled[at, :].astype(F32) * columns[:, block : block + 1]).astype(BF16)

    def launch_first(i):
        send(first_send.at[2 * i], first_got.at[2 * i], first_sem, at_x(flip), i)
        send(first_send.at[2 * i + 1], first_got.at[2 * i + 1], first_sem, at_x(back), i)

    def compute(*blocks):
        at = slice(blocks[0] * NX * OWNED, (blocks[-1] + 1) * NX * OWNED)
        product = [
            jnp.dot(table[at, :], weighted[:, i * HALF : (i + 1) * HALF], preferred_element_type=F32) for i in range(2)
        ]
        sends = []
        for k, i in enumerate(blocks):
            block = product[1][k * NX * OWNED : (k + 1) * NX * OWNED]
            for colour, keeps, keep, device in ((0, (1, 3, 5, 7), keep_c, at_z(-away)), (1, (2, 4, 6, 7), keep_d, at_z(away))):
                part = block[:, colour * QUARTER : (colour + 1) * QUARTER]
                if i in keeps:
                    keep[keeps.index(i)] = part
                else:
                    n = [j for j in range(NZ) if j not in keeps].index(i)
                    slot = 2 * n + colour
                    pair_send[slot] = part.astype(BF16)
                    sends.append((slot, n, device))
            block = product[0][k * NX * OWNED : (k + 1) * NX * OWNED]
            g = [slice(j * OWNED, (j + 1) * OWNED) for j in range(NX)]
            if i in DIRECT:
                n = DIRECT.index(i)
                keep_w[n] = block[g[0]]
                direct_send[3 * n] = block[g[1]].astype(BF16)
                direct_send[3 * n + 1] = block[g[2]].astype(BF16)
                direct_send[3 * n + 2] = block[g[3]].astype(BF16)
                continue
            keep_a[i, :OWNED, :] = block[g[0], :QUARTER]
            keep_a[i, OWNED:, :] = block[g[2], :QUARTER]
            first_send[2 * i, :OWNED, :] = block[g[1], :QUARTER].astype(BF16)
            first_send[2 * i, OWNED:, :] = block[g[3], :QUARTER].astype(BF16)
            keep_b[i] = block[: 2 * OWNED, QUARTER:]
            first_send[2 * i + 1] = block[2 * OWNED :, QUARTER:].astype(BF16)
        for slot, n, device in sends:
            send(pair_send.at[slot], pair_got.at[slot], pair_sem, device, n)

    def launch_x(i):
        if i not in DIRECT:
            launch_first(i)
            return
        n = DIRECT.index(i)
        for j, other in ((2, across), (0, flip), (1, back)):
            send(direct_send.at[3 * n + j], direct_got.at[3 * n + j], direct_sem, at_x(other), n)

    def after_direct(i):
        n = DIRECT.index(i)
        landed(direct_got.at[3 * n : 3 * n + 3], direct_sem, n)
        result = keep_w[n]
        for j in range(3):
            result = result + direct_got[3 * n + j].astype(F32)
        return result[:, :QUARTER], result[:, QUARTER:]

    def after_pair(n):
        landed(pair_got.at[2 * n : 2 * n + 2], pair_sem, n)
        i = NZ + n
        c, d = 2 * n, 2 * n + 1
        first_send[2 * i, :OWNED, :] = (keep_c[n, OWNED : 2 * OWNED, :] + pair_got[c, OWNED : 2 * OWNED, :].astype(F32)).astype(BF16)
        first_send[2 * i, OWNED:, :] = (keep_c[n, 3 * OWNED :, :] + pair_got[c, 3 * OWNED :, :].astype(F32)).astype(BF16)
        first_send[2 * i + 1] = (keep_d[n, 2 * OWNED :, :] + pair_got[d, 2 * OWNED :, :].astype(F32)).astype(BF16)
        launch_first(i)
        keep_a[i, :OWNED, :] = keep_c[n, :OWNED, :] + pair_got[c, :OWNED, :].astype(F32)
        keep_a[i, OWNED:, :] = keep_c[n, 2 * OWNED : 3 * OWNED, :] + pair_got[c, 2 * OWNED : 3 * OWNED, :].astype(F32)
        keep_b[i] = keep_d[n, : 2 * OWNED, :] + pair_got[d, : 2 * OWNED, :].astype(F32)

    def after_first(i):
        landed(first_got.at[2 * i : 2 * i + 2], first_sem, i)
        second_send[2 * i] = (keep_a[i, OWNED:, :] + first_got[2 * i, OWNED:, :].astype(F32)).astype(BF16)
        second_send[2 * i + 1] = (keep_b[i, OWNED:, :] + first_got[2 * i + 1, OWNED:, :].astype(F32)).astype(BF16)
        send(second_send.at[2 * i], second_got.at[2 * i], second_sem, at_x(back), i)
        send(second_send.at[2 * i + 1], second_got.at[2 * i + 1], second_sem, at_x(flip), i)

    def after_second(i):
        landed(second_got.at[2 * i : 2 * i + 2], second_sem, i)
        return (
            keep_a[i, :OWNED, :] + first_got[2 * i, :OWNED, :].astype(F32) + second_got[2 * i].astype(F32),
            keep_b[i, :OWNED, :] + first_got[2 * i + 1, :OWNED, :].astype(F32) + second_got[2 * i + 1].astype(F32),
        )

    def wide(i):
        sum_a, sum_b = after_direct(i) if i in DIRECT else after_second(i)
        wide_send[i, :, :QUARTER] = sum_a.astype(BF16)
        wide_send[i, :, QUARTER:] = sum_b.astype(BF16)
        offset = (NZ - 1 - i) // 2 if i % 2 else -((NZ - i) // 2)
        send(wide_send.at[i], wide_got.at[i], wide_sem, at_z(away * offset))

    def at_far(other, step):
        return {"ex": other * NZ + (z + step + 2 * NZ) % NZ}

    def slim(n):
        i = NZ + n
        landed(first_got.at[2 * i : 2 * i + 2], first_sem, i)
        sum_c = keep_a[i] + first_got[2 * i].astype(F32)
        sum_d = keep_b[i] + first_got[2 * i + 1].astype(F32)
        ahead = away * (NX - 1 - n)
        routes = [(sum_c[OWNED:], back, ahead), (sum_d[OWNED:], flip, -ahead), (sum_c[:OWNED], x, ahead), (sum_d[:OWNED], x, -ahead)]
        for j, (part, other, step) in enumerate(routes[: 2 if n == NX - 1 else 4]):
            slim_send[4 * n + j] = part.astype(BF16)
            send(slim_send.at[4 * n + j], slim_got.at[4 * n + j], slim_sem, at_far(other, step))
        return sum_c[:OWNED], sum_d[:OWNED]

    compute(0)
    launch_x(0)
    compute(1, 2)
    launch_x(1)
    launch_x(2)
    compute(3, 4)
    launch_x(3)
    launch_x(4)
    compute(5, 6)
    launch_x(5)
    launch_x(6)
    compute(7)
    flat = jnp.concatenate([residual[i : i + 1, :] for i in range(BLOCKS)], axis=1).astype(BF16)
    grad = jnp.dot(jnp.broadcast_to(flat, (8, ROWS)), pooled[...], preferred_element_type=F32)[0:1, :]
    for i in range(NX):
        xgrad_send[i] = grad[:, i * LANES : (i + 1) * LANES]
    for step in (2, 1, 3):
        send(xgrad_send.at[(x + step) % NX], xgrad.at[step], xgrad_sem, at_x((x + step) % NX))
    after_pair(0)
    wide(0)
    after_pair(1)
    wide(1)
    after_first(3)
    after_pair(2)
    after_first(4)
    after_first(5)
    wide(2)
    after_pair(3)
    launch_x(7)
    after_first(6)
    slim(0)
    landed(xgrad.at[1:], xgrad_sem)
    part = xgrad_send[x]
    for step in range(1, NX):
        part = part + xgrad[step]
    zgrad_send[...] = part
    for step in FAR_FIRST:
        send(zgrad_send, zgrad.at[step], zgrad_sem, at_z(step))
    wide(3)
    slim(1)
    wide(4)
    slim(2)
    wide(5)
    sum_c, sum_d = slim(3)
    wide(6)
    sum_a, sum_b = after_direct(NZ - 1)
    landed(zgrad.at[1:], zgrad_sem)
    part = zgrad_send[...]
    for step in range(1, NZ):
        part = part + zgrad[step]
    grad_out[...] = pltpu.roll(part, (NZ - z) * 16 % LANES, 1)[:, :16] * (1.0 / 256.0)
    landed(wide_got, wide_sem)
    for i in range(NZ - 1):
        sum_a = sum_a + wide_got[i, :, :QUARTER].astype(F32)
        sum_b = sum_b + wide_got[i, :, QUARTER:].astype(F32)
    landed(slim_got, slim_sem)
    for slot in range(0, 4 * NX - 2, 2):
        sum_c = sum_c + slim_got[slot].astype(F32)
        sum_d = sum_d + slim_got[slot + 1].astype(F32)
    for i, part in enumerate((sum_a, sum_b, sum_c, sum_d)):
        sketch_out[:, i * QUARTER : (i + 1) * QUARTER] = part * (1.0 / 32.0)
    left(zdir.at[1:], zdir_sem)
    left(xdir.at[1:], xdir_sem)
    left(terms.at[1:], terms_sem)
    left(xgrad.at[1:], xgrad_sem)
    left(zgrad.at[1:], zgrad_sem)
    left(pair_send, pair_sem)
    left(first_send.at[: 2 * (NX + NZ - len(DIRECT))], first_sem)
    left(second_send.at[: 2 * (NZ - len(DIRECT))], second_sem)
    left(direct_send, direct_sem)
    left(wide_send, wide_sem)
    left(slim_send, slim_sem)


def put_out(margins, grad, sketch, margins_hbm, grad_hbm, sketch_hbm, sem):
    copies = [
        pltpu.make_async_copy(src, dst, sem.at[i])
        for i, (src, dst) in enumerate(((sketch, sketch_hbm), (margins, margins_hbm), (grad, grad_hbm)))
    ]
    for copy in copies:
        copy.start()
    for copy in copies:
        copy.wait()


def on_device(pooled, labels, sign_bits, margins_old, direction, sample_rows):
    dma = pltpu.SemaphoreType.DMA
    vmem = pltpu.VMEM
    margins, grad, sketch = pl.pallas_call(
        kernel,
        out_shape=(
            jax.ShapeDtypeStruct((BLOCKS, LANES), F32),
            jax.ShapeDtypeStruct((1, 16), F32),
            jax.ShapeDtypeStruct((OWNED, COLS), F32),
        ),
        in_specs=[pl.BlockSpec(memory_space=pl.ANY)] * 6,
        out_specs=[pl.BlockSpec(memory_space=vmem)] * 3,
        scratch_shapes=[
            vmem((ROWS, COLS), BF16),
            vmem((BLOCKS, LANES), jnp.int32),
            vmem((BLOCKS, LANES), jnp.int32),
            vmem((BLOCKS, LANES), F32),
            vmem((1, 16), F32),
            vmem((SAMPLES // LANES, LANES), jnp.int32),
            vmem((SAMPLES, LANES), jnp.int32),
            vmem((SAMPLES, ROWS), BF16),
            vmem((ROWS, COLS), BF16),
            vmem((NZ, 1, LANES), F32),
            vmem((NX, 1, LANES), F32),
            vmem((NF, BLOCKS, LANES), BF16),
            vmem((NX, 1, LANES), F32),
            vmem((NX, 1, LANES), F32),
            vmem((1, LANES), F32),
            vmem((NZ, 1, LANES), F32),
            vmem((NZ + NX, 2 * OWNED, QUARTER), F32),
            vmem((NZ + NX, 2 * OWNED, QUARTER), F32),
            vmem((NX, NX * OWNED, QUARTER), F32),
            vmem((NX, NX * OWNED, QUARTER), F32),
            vmem((2 * NX, NX * OWNED, QUARTER), BF16),
            vmem((2 * NX, NX * OWNED, QUARTER), BF16),
            vmem((2 * (NZ + NX), 2 * OWNED, QUARTER), BF16),
            vmem((2 * (NZ + NX), 2 * OWNED, QUARTER), BF16),
            vmem((2 * NZ, OWNED, QUARTER), BF16),
            vmem((2 * NZ, OWNED, QUARTER), BF16),
            vmem((NZ - 1, OWNED, 2 * QUARTER), BF16),
            vmem((NZ - 1, OWNED, 2 * QUARTER), BF16),
            vmem((4 * NX - 2, OWNED, QUARTER), BF16),
            vmem((4 * NX - 2, OWNED, QUARTER), BF16),
            vmem((len(DIRECT), OWNED, HALF), F32),
            vmem((3 * len(DIRECT), OWNED, HALF), BF16),
            vmem((3 * len(DIRECT), OWNED, HALF), BF16),
            dma((6,)),
            dma((2,)),
            dma((NX,)),
            dma((2,)),
            dma((2,)),
            dma((2,)),
            dma((1 + NX,)),
            dma((1 + NZ + NX,)),
            dma((1 + NZ,)),
            dma((2,)),
            dma((2,)),
            dma((1 + len(DIRECT),)),
        ],
        compiler_params=pltpu.CompilerParams(vmem_limit_bytes=40 << 20, collective_id=0, has_side_effects=True),
        name="newton_sketch",
    )(*(pltpu.with_memory_space_constraint(array, pltpu.HBM) for array in (
        pooled,
        labels.reshape(BLOCKS, LANES),
        sign_bits.reshape(BLOCKS, LANES),
        margins_old.reshape(BLOCKS, LANES),
        direction.reshape(1, 16),
        sample_rows.reshape(SAMPLES // LANES, LANES),
    )))
    margins, grad, sketch = pl.pallas_call(
        put_out,
        out_shape=(
            jax.ShapeDtypeStruct((BLOCKS, LANES), F32),
            jax.ShapeDtypeStruct((1, 16), F32),
            jax.ShapeDtypeStruct((OWNED, COLS), F32),
        ),
        in_specs=[pl.BlockSpec(memory_space=vmem)] * 3,
        out_specs=[pl.BlockSpec(memory_space=pl.ANY)] * 3,
        scratch_shapes=[dma((3,))],
        compiler_params=pltpu.CompilerParams(vmem_limit_bytes=1 << 20),
        name="put_out",
    )(margins, grad, sketch)
    return margins.reshape(ROWS), grad.reshape(16), sketch


def solution(mesh):
    return jax.shard_map(
        on_device,
        mesh=mesh,
        in_specs=(P("ex", "feat"), P("ex"), P("ex"), P("ex"), P(("feat", "ex")), P()),
        out_specs=(P("ex"), P(("feat", "ex")), P("ex", "feat")),
        check_vma=False,
    )
```
